1024 devices in a mesh: expert: 64 (over z, x_hi, core), mp: 16 (over y, x_lo).
Axes of the slice: x: 4 (x_hi: 2, x_lo: 2; x = x_hi * 2 + x_lo), y: 8, z: 16, core: 2. Of those that a mesh axis runs over, the one named last changes fastest.
Arguments:
- tokens: bfloat16 [2, 20480, 2048], P(None, 'expert', 'mp'), may hold values from -6 to 6
- expert_index: int32 [2, 20480], P(None, 'expert'), may hold values from 0 to 63
- slot_index: int32 [2, 20480], P(None, 'expert'), may hold values from 0 to 5, as said below
- kept_mask: int32 [2, 20480], P(None, 'expert'), may hold values from 0 to 1
- gate_prob: float32 [2, 20480], P(None, 'expert'), may hold values from 0.2 to 1
- w_in: bfloat16 [64, 2048, 6144], P('expert', None, 'mp'), may hold values from -0.125 to 0.125
- w_out: bfloat16 [64, 6144, 2048], P('expert', 'mp'), may hold values from -0.078125 to 0.078125
Outputs:
- mixed: bfloat16 [2, 20480, 2048], P(None, 'expert', 'mp')
The draws below stay inside these ranges and needn't reach their ends.
Inputs may be any that keep to these rules, and one draw needn't show every extreme that they name: `slot_index`: within one aligned block of 320 tokens of a group, no two kept tokens share both expert and slot; in every group some expert has all 6 slots of every block taken. Dropped tokens carry a slot value too, which means nothing.
All inputs are finite; a program needn't handle non-finite values.
Results may differ from the reference program's by a relative error of at most 0.018.
Values may be sent and summed in bfloat16 or wider, within the bound.
A program may use at most 32 MiB of HBM per device.

```python
import jax
import jax.numpy as jnp
from jax import lax

D = 2048
FF = 6144
GROUPS = 2
TOK_GRP = 320
CAP = 6
EXPERTS = 64
TOKENS = 20480
N_EXPERT = 64
N_MP = 16


def routing(key):
    base = jax.random.fold_in(key, 7)
    first_key, second_key, third_key = jax.random.split(base, 3)
    blocks = GROUPS * (TOKENS // TOK_GRP)
    favored = jax.random.randint(first_key, (GROUPS, 1), 0, EXPERTS)
    favored = jnp.repeat(favored, TOKENS // TOK_GRP, axis=0)
    picks = jax.random.randint(second_key, (blocks, TOK_GRP), 0, EXPERTS)
    scores = jax.random.randint(third_key, (blocks, TOK_GRP), 0, 2 ** 20)
    scores = scores * TOK_GRP + jnp.arange(TOK_GRP, dtype=jnp.int32)[None, :]
    ranking = jnp.argsort(jnp.argsort(scores, axis=1), axis=1)
    chosen = jnp.where(ranking < 2 * CAP, favored, picks).astype(jnp.int32)
    onehot = (chosen[:, :, None] == jnp.arange(EXPERTS, dtype=jnp.int32)[None, None, :]).astype(jnp.int32)
    before = jnp.cumsum(onehot, axis=1) - onehot
    position = jnp.sum(before * onehot, axis=2)
    kept = (position < CAP).astype(jnp.int32)
    slot = (position % CAP).astype(jnp.int32)
    return (chosen.reshape(GROUPS, TOKENS), slot.reshape(GROUPS, TOKENS), kept.reshape(GROUPS, TOKENS))


def draw_expert_index(key, part):
    return routing(key)[0]


def draw_slot_index(key, part):
    return routing(key)[1]


def draw_kept_mask(key, part):
    return routing(key)[2]


def block_levels(rng, dims, pieces, low, high):
    def one(dim, shards_of):
        steps = jax.random.uniform(jax.random.fold_in(jax.random.fold_in(rng, 6), dim), (shards_of,), jnp.float32, low / len(pieces), high / len(pieces))
        return jnp.repeat(jnp.exp(steps), dims[dim] // shards_of).reshape((-1,) + (1,) * (len(dims) - dim - 1))

    gain = one(*pieces[0])
    for cut in pieces[1:]:
        gain = gain * one(*cut)
    return gain


def centred(stream_key, dims, scale, bound, shards=(), held_as=jnp.bfloat16):
    entries = jax.random.normal(stream_key, dims, jnp.float32) * scale
    if len(shards) > 0:
        entries = block_levels(stream_key, dims, shards, -0.22, 0.18) * entries
    return jnp.clip(entries, min=-bound, max=bound).astype(held_as)


def setup_inputs(seed: int = 0) -> dict:
    seeds = jax.random.split(jax.random.key(seed), 8)
    tokens = centred(seeds[0], (GROUPS, TOKENS, D), 1.0, 6.0, ((1, 64), (2, 16)))
    expert_index = draw_expert_index(jax.random.fold_in(seeds[7], 71), 0)
    slot_index = draw_slot_index(jax.random.fold_in(seeds[7], 71), 0)
    kept_mask = draw_kept_mask(jax.random.fold_in(seeds[7], 71), 0)
    gate_prob = jnp.clip(0.2 + 0.8 * jax.random.uniform(seeds[4], (GROUPS, TOKENS), jnp.float32) ** block_levels(seeds[4], (GROUPS, TOKENS), ((1, 64),), -0.2, 0.2), 0.2, 1.0)
    w_in = centred(seeds[5], (EXPERTS, D, FF), D ** -0.5, 0.125, ((0, 64), (2, 16)))
    w_out = centred(seeds[6], (EXPERTS, FF, D), FF ** -0.5, 0.078125, ((0, 64), (1, 16)))
    return dict(tokens=tokens, expert_index=expert_index, slot_index=slot_index, kept_mask=kept_mask, gate_prob=gate_prob, w_in=w_in, w_out=w_out)


def reference(tokens, expert_index, slot_index, kept_mask, gate_prob, w_in, w_out):
    rows_each = N_EXPERT * CAP
    width = FF // N_MP
    source = (jnp.arange(TOKENS, dtype=jnp.int32) // TOK_GRP).astype(jnp.int32)

    def expert_work(args):
        block, first, second = args
        pre = jnp.dot(block, first, preferred_element_type=jnp.float32)
        hidden = jnp.maximum(pre, 0.0).astype(jnp.bfloat16)
        total = jnp.zeros((rows_each, D), jnp.float32)
        for k in range(N_MP):
            part = jnp.dot(hidden[:, k * width:(k + 1) * width], second[k * width:(k + 1) * width],
                           preferred_element_type=jnp.float32).astype(jnp.bfloat16)
            part = lax.optimization_barrier(part)
            total = total + part.astype(jnp.float32)
        return total.astype(jnp.bfloat16)

    results = []
    for group in range(GROUPS):
        place = expert_index[group] * rows_each + source * CAP + slot_index[group]
        place = jnp.where(kept_mask[group] > 0, place, EXPERTS * rows_each).astype(jnp.int32)
        buffer = jnp.zeros((EXPERTS * rows_each + 1, D), jnp.bfloat16).at[place].set(tokens[group])
        buffer = buffer[:-1].reshape(EXPERTS, rows_each, D)
        done = lax.map(expert_work, (buffer, w_in, w_out)).reshape(EXPERTS * rows_each, D)
        picked = done[jnp.minimum(place, EXPERTS * rows_each - 1).astype(jnp.int32)].astype(jnp.float32)
        mixed = jnp.where(kept_mask[group][:, None] > 0, gate_prob[group][:, None] * picked, 0.0)
        results.append(mixed.astype(jnp.bfloat16))
    return jnp.stack(results)
```

```python
import jax
import jax.numpy as jnp
from jax import lax
from jax.experimental import pallas as pl
from jax.experimental.pallas import tpu as pltpu
from jax.sharding import Mesh
from jax.sharding import PartitionSpec as P

GROUPS = 2
CAP = 6
EXPERT = ("expert_0", "expert_1", "expert_2")
MP = ("mp_0", "mp_1")
MESH = pl.DeviceIdType.MESH
NY = 8
HALF = NY // 2
PLUS, MINUS = 0, 1


def cut_along(value, dim, count):
    before, after = (value.shape[:dim], value.shape[dim + 1 :])
    return jnp.moveaxis(value.reshape(*before, count, -1, *after), dim, 0)


def laid_out(blocks, dim):
    blocks = jnp.moveaxis(blocks, 0, dim)
    dims = blocks.shape
    return blocks.reshape(*dims[:dim], dims[dim] * dims[dim + 1], *dims[dim + 2 :])


def moved_by_axis(blocks, axes, order):
    inside = blocks.shape[1:]
    filled = blocks.reshape(*(lax.axis_size(a) for a in axes), *inside)
    for k in order:
        filled = lax.all_to_all(filled, axes[k], k, k, tiled=True)
    return filled.reshape(-1, *inside)


def two_step_exchange(value, groups, order, split_dim, concat_dim):
    count = lax.axis_size(groups[0]) * lax.axis_size(groups[1])
    blocks = cut_along(value, split_dim, count)
    return laid_out(moved_by_axis(blocks, groups, order), concat_dim)


def slot_table(expert_index, slot_index, kept_mask, experts):
    code = jnp.where(kept_mask > 0, expert_index * CAP + slot_index, -1)
    places = lax.broadcasted_iota(jnp.int32, (experts * CAP, code.shape[0]), 0)
    return (places == code[None, :]).astype(jnp.bfloat16)


GATHER = ((0, 1), (0, 0), (1, 0))
REDUCE = ((1, 0), (0, 0), (0, 1))


def row_range(piece, direction, distance, rows):
    column, half = piece
    start, size = half * (rows // 2), rows // 2
    if distance < HALF:
        return start, size
    if piece == (0, 0):
        return (start, size) if direction == PLUS else None
    if piece == (0, 1):
        return (start, size) if direction == MINUS else None
    part = size // 2
    return (start, part) if direction == PLUS else (start + part, size - part)


def expert_kernel(
    x_ref, win_hbm, wout_hbm, out_ref,
    win, wout, load_sem, gath, pre, hidden,
    gy_send, gy_recv, gx_send, gx_recv,
    ry_buf, ry_out, rx_buf, rx_out,
    ry_send, ry_recv, rx_send, rx_recv,
):
    rows, width = x_ref.shape
    half = rows // 2
    y = lax.axis_index("mp_0")
    c = lax.axis_index("mp_1")
    up = lax.rem(y + 1, NY)
    down = lax.rem(y + NY - 1, NY)
    ring = ({"mp_0": up}, {"mp_0": down})
    across = {"mp_1": 1 - c}

    first = pltpu.make_async_copy(win_hbm.at[0], win, load_sem.at[0])
    second = pltpu.make_async_copy(wout_hbm.at[0], wout, load_sem.at[1])
    first.start()
    second.start()

    barrier = pltpu.get_barrier_semaphore()
    for device in (ring[0], ring[1], across):
        pl.semaphore_signal(barrier, inc=1, device_id=device, device_id_type=MESH)
    pl.semaphore_wait(barrier, 3)

    def feature(r, column):
        place = lax.rem(y + r, NY) * 2 + (c if column == 0 else 1 - c)
        return pl.ds(pl.multiple_of(place * width, width), width)

    sent = []

    def push(src, dst, send_sem, recv_sem, device):
        copy = pltpu.make_async_remote_copy(
            src_ref=src, dst_ref=dst, send_sem=send_sem, recv_sem=recv_sem,
            device_id=device, device_id_type=MESH,
        )
        copy.start()
        sent.append(copy)

    def arrived(dst, recv_sem, send_sem):
        pltpu.make_async_remote_copy(
            src_ref=dst, dst_ref=dst, send_sem=send_sem, recv_sem=recv_sem,
            device_id=across, device_id_type=MESH,
        ).wait_recv()

    def held(r, column, start, size):
        if r == 0 and column == 0:
            return x_ref.at[pl.ds(start, size)]
        return gath.at[r, column, pl.ds(start, size)]

    def ring_slot(direction, distance):
        return (NY - distance) if direction == PLUS else distance

    def gather_send(direction, distance, p):
        span = row_range(GATHER[p], direction, distance, rows)
        if span is None:
            return
        column = GATHER[p][0]
        here = 0 if distance == 1 else ring_slot(direction, distance - 1)
        there = ring_slot(direction, distance)
        push(
            held(here, column, *span),
            gath.at[there, column, pl.ds(*span)],
            gy_send.at[direction, distance - 1, p],
            gy_recv.at[direction, distance - 1, p],
            ring[direction],
        )

    def cross_send(r):
        push(
            held(r, 0, half, half), gath.at[r, 1, pl.ds(half, half)],
            gx_send.at[r], gx_recv.at[r], across,
        )

    def cross_wait(r):
        arrived(gath.at[r, 1, pl.ds(half, half)], gx_recv.at[r], gx_send.at[r])

    def fold(r, column, start, size, first_time=False):
        piece = held(r, column, start, size)[...]
        part = jnp.dot(piece, win[feature(r, column), :], preferred_element_type=jnp.float32)
        if first_time:
            pre[pl.ds(start, size), :] = part
        else:
            pre[pl.ds(start, size), :] += part

    push(
        held(0, 0, 0, half), gath.at[0, 1, pl.ds(0, half)],
        gx_send.at[NY], gx_recv.at[NY], across,
    )
    for p in (0, 1):
        gather_send(PLUS, 1, p)
        gather_send(MINUS, 1, p)
    cross_send(0)
    first.wait()
    fold(0, 0, 0, half, True)
    arrived(gath.at[0, 1, pl.ds(0, half)], gx_recv.at[NY], gx_send.at[NY])
    gather_send(PLUS, 1, 2)
    gather_send(MINUS, 1, 2)
    fold(0, 0, half, half, True)
    fold(0, 1, 0, half)
    for distance in range(1, HALF + 1):
        for p in range(3):
            column, part_half = GATHER[p]
            for direction in (PLUS, MINUS):
                span = row_range(GATHER[p], direction, distance, rows)
                if span is None:
                    continue
                r = ring_slot(direction, distance)
                arrived(
                    gath.at[r, column, pl.ds(*span)],
                    gy_recv.at[direction, distance - 1, p],
                    gy_send.at[direction, distance - 1, p],
                )
                if distance < HALF:
                    gather_send(direction, distance + 1, p)
                if (column, part_half) == (0, 1):
                    cross_send(r)
                fold(r, column, *span)
        for r in ((0,) if distance == 1 else (NY - distance + 1, distance - 1)):
            cross_wait(r)
            fold(r, 1, half, half)
    cross_wait(HALF)
    fold(HALF, 1, half, half)
    for copy in sent:
        copy.wait_send()
    sent.clear()

    hidden[...] = jnp.maximum(pre[...], 0.0).astype(jnp.bfloat16)
    second.wait()

    def block(r, column, start, size):
        return jnp.dot(
            hidden[pl.ds(start, size), :], wout[:, feature(r, column)],
            preferred_element_type=jnp.float32,
        )

    def cross_term(r):
        rx_out[r] = block(r, 1, half, half).astype(jnp.bfloat16)
        push(rx_out.at[r], rx_buf.at[r], rx_send.at[r], rx_recv.at[r], across)

    def cross_arrived(r):
        arrived(rx_buf.at[r], rx_recv.at[r], rx_send.at[r])

    def ring_arrived(direction, distance, p, span):
        slot = ry_buf.at[direction, distance, p, pl.ds(span[0] % half, span[1])]
        arrived(slot, ry_recv.at[direction, distance, p], ry_send.at[direction, distance, p])
        return slot

    def reduce_send(direction, distance, p):
        piece = REDUCE[p]
        r = distance if direction == PLUS else NY - distance
        full = row_range(piece, direction, distance, rows)
        if full is None:
            return
        total = block(r, piece[0], *full)
        if piece == (0, 1):
            total = total + rx_buf[r].astype(jnp.float32)
        out = ry_out.at[direction, distance - 1, p, pl.ds(full[0] % half, full[1])]
        if distance < HALF:
            coming = row_range(piece, direction, distance + 1, rows)
            if coming is not None:
                slot = ring_arrived(direction, distance, p, coming)
                if coming == full:
                    total = total + slot[...].astype(jnp.float32)
                else:
                    low = coming[0] - full[0]
                    parts = []
                    if low > 0:
                        parts.append(total[:low])
                    parts.append(total[low : low + coming[1]] + slot[...].astype(jnp.float32))
                    if low + coming[1] < full[1]:
                        parts.append(total[low + coming[1] :])
                    total = jnp.concatenate(parts, axis=0)
        out[...] = total.astype(jnp.bfloat16)
        push(
            out, ry_buf.at[direction, distance - 1, p, pl.ds(full[0] % half, full[1])],
            ry_send.at[direction, distance - 1, p], ry_recv.at[direction, distance - 1, p],
            ring[direction],
        )

    cross_term(HALF)
    for p in (0, 1):
        reduce_send(PLUS, HALF, p)
        reduce_send(MINUS, HALF, p)
    cross_term(HALF - 1)
    cross_term(HALF + 1)
    cross_arrived(HALF)
    reduce_send(MINUS, HALF, 2)
    for distance in range(HALF - 1, 0, -1):
        for r in ((distance - 1, NY - distance + 1) if distance > 1 else (0,)):
            cross_term(r)
        for p in range(3):
            if p == 2:
                cross_arrived(distance)
                cross_arrived(NY - distance)
            for direction in (PLUS, MINUS):
                reduce_send(direction, distance, p)

    def last(p):
        piece = REDUCE[p]
        start = piece[1] * half
        total = block(0, piece[0], start, half)
        for direction in (PLUS, MINUS):
            total = total + ring_arrived(direction, 0, p, (start, half))[...].astype(jnp.float32)
        return total

    rx_out[NY] = last(0).astype(jnp.bfloat16)
    push(rx_out.at[NY], rx_buf.at[NY], rx_send.at[NY], rx_recv.at[NY], across)
    upper = last(1)
    cross_arrived(0)
    lower = last(2) + rx_buf[0].astype(jnp.float32)
    out_ref[pl.ds(half, half), :] = lower.astype(jnp.bfloat16)
    cross_arrived(NY)
    out_ref[pl.ds(0, half), :] = (upper + rx_buf[NY].astype(jnp.float32)).astype(jnp.bfloat16)
    for copy in sent:
        copy.wait_send()


def expert_pass(x, w_in, w_out):
    rows, width = x.shape
    half = rows // 2
    bf16, f32 = jnp.bfloat16, jnp.float32
    dma = pltpu.SemaphoreType.DMA
    return pl.pallas_call(
        expert_kernel,
        out_shape=jax.ShapeDtypeStruct((rows, width), bf16),
        in_specs=[
            pl.BlockSpec(memory_space=pltpu.VMEM),
            pl.BlockSpec(memory_space=pl.ANY),
            pl.BlockSpec(memory_space=pl.ANY),
        ],
        out_specs=pl.BlockSpec(memory_space=pltpu.VMEM),
        scratch_shapes=[
            pltpu.VMEM(w_in.shape[1:], bf16),
            pltpu.VMEM(w_out.shape[1:], bf16),
            dma((2,)),
            pltpu.VMEM((NY, 2, rows, width), bf16),
            pltpu.VMEM((rows, w_in.shape[2]), f32),
            pltpu.VMEM((rows, w_in.shape[2]), bf16),
            dma((2, HALF, 3)), dma((2, HALF, 3)), dma((NY + 1,)), dma((NY + 1,)),
            pltpu.VMEM((2, HALF, 3, half, width), bf16),
            pltpu.VMEM((2, HALF, 3, half, width), bf16),
            pltpu.VMEM((NY + 1, half, width), bf16),
            pltpu.VMEM((NY + 1, half, width), bf16),
            dma((2, HALF, 3)), dma((2, HALF, 3)), dma((NY + 1,)), dma((NY + 1,)),
        ],
        compiler_params=pltpu.CompilerParams(
            collective_id=0, has_side_effects=True, vmem_limit_bytes=48 * 1024 * 1024
        ),
        name="expert_ring",
    )(x, w_in, w_out)


def combine(table, returned, gate):
    flat = returned.reshape(returned.shape[0] * returned.shape[1], returned.shape[2])
    picked = lax.dot_general(
        table, flat, (((0,), (0,)), ((), ())), preferred_element_type=jnp.float32
    )
    return (gate[:, None] * picked).astype(jnp.bfloat16)


def on_device(tokens, expert_index, slot_index, kept_mask, gate_prob, w_in, w_out):
    experts = lax.axis_size(EXPERT)
    narrow = tokens.shape[2]
    tables = []
    outgoing = []
    for group in range(GROUPS):
        table = slot_table(expert_index[group], slot_index[group], kept_mask[group], experts)
        tables.append(table)
        packed = jnp.dot(table, tokens[group], preferred_element_type=jnp.float32).astype(
            jnp.bfloat16
        )
        outgoing.append(packed.reshape(experts, CAP, narrow))
    results = []
    stacked = jnp.concatenate(outgoing, axis=1)
    split = (("expert_0", "expert_1"), "expert_2")
    received = two_step_exchange(stacked, split, (1, 0), 0, 0)
    source, slots, _ = received.shape
    summed = expert_pass(received.reshape(source * slots, narrow), w_in, w_out)
    returned = two_step_exchange(summed.reshape(source, slots, narrow), split, (1, 0), 0, 0)
    for group in range(GROUPS):
        own = returned[:, group * CAP : (group + 1) * CAP, :]
        results.append(combine(tables[group], own, gate_prob[group]))
    return jnp.stack(results)


def solution(mesh):
    torus = Mesh(
        mesh.devices.reshape(16, 2, 2, 8, 2), ("expert_0", "expert_1", "expert_2", "mp_0", "mp_1")
    )
    placed = (
        P(None, EXPERT, MP),
        P(None, EXPERT),
        P(None, EXPERT),
        P(None, EXPERT),
        P(None, EXPERT),
        P(EXPERT, None, MP),
        P(EXPERT, MP, None),
    )
    return jax.shard_map(
        on_device, mesh=torus, in_specs=placed, out_specs=P(None, EXPERT, MP), check_vma=False
    )
```
